32 devices in a mesh: grp: 8 (over y, x, core), rest: 4 (over z).
Axes of the slice: x: 2, y: 2, z: 4, core: 2. Of those that a mesh axis runs over, the one named last changes fastest.
Arguments:
- grads: bfloat16 [8, 9216, 1024], P('grp', 'rest'), parts along dimension 1, may hold values from -6 to 6
- weight: bfloat16 [9216, 1024], P('rest'), parts along dimension 0, may hold values from -0.625 to 0.625
- moment1: float32 [2304, 4096], P('grp', 'rest'), parts along dimension 1, may hold values from -2 to 2
- moment2: float32 [2304, 4096], P('grp', 'rest'), parts along dimension 1, may hold values from 0.0001 to 0.04
- step: int32 [1], replicated, may hold values from 1 to 8
Outputs:
- new_weight: bfloat16 [9216, 1024], P('rest'), parts along dimension 0
- new_moment1: float32 [2304, 4096], P('grp', 'rest'), parts along dimension 1
- new_moment2: float32 [2304, 4096], P('grp', 'rest'), parts along dimension 1
The draws below stay inside these ranges and needn't reach their ends.
There are 4 independent parts, one for each index of `rest`. The reference program is written for one: setup_inputs(seed, part) draws one part's arguments, and reference() takes and returns one part's arrays. A program takes and returns all parts, laid end to end along the dimension named above; an argument that names none is the same for every part. Nothing has to cross between parts.
All inputs are finite; a program needn't handle non-finite values.
Results may differ from the reference program's by a relative error of at most 0.006.
Values may be sent and summed in bfloat16 or wider, within the bound.
No kernel may reach another device: no remote copies, remote signals or barrier semaphores. Data moves between devices by JAX's collectives and lax.ppermute only.
A program may use at most 128 MiB of HBM per device.

```python
import math
import jax
import jax.numpy as jnp
from jax import lax

D = 2304
KV = 1024
N_GRP = 8


def spiked(result, key, source, target, blocks, factor):
    owner, partner = [(jnp.arange(result.shape[position]) // (result.shape[position] // blocks)).reshape([-1 if axis == position else 1 for axis in range(result.ndim)]) for position in (source, target)]
    chosen = jax.random.permutation(key, blocks)[partner]
    strong = (owner == chosen) | (owner == (partner + blocks // 2) % blocks)
    return jnp.where(strong, factor * result, result)


def shard_levels(rng, dims, pieces, least, top_value):
    def one(position, blocks):
        steps = jax.random.uniform(jax.random.fold_in(jax.random.fold_in(rng, 6), position), (blocks,), jnp.float32, least / len(pieces), top_value / len(pieces))
        return jnp.repeat(jnp.exp(steps), dims[position] // blocks).reshape((-1,) + (1,) * (len(dims) - position - 1))

    loudness = one(*pieces[0])
    for cut in pieces[1:]:
        loudness = loudness * one(*cut)
    return loudness


def centred(stream_key, dims, spread, reach, cuts=(), dtype=jnp.bfloat16):
    drawn = spread * jax.random.normal(stream_key, dims, jnp.float32)
    if cuts:
        drawn = drawn * shard_levels(stream_key, dims, cuts, -0.22, 0.18)
    return jnp.clip(drawn, -reach, reach).astype(dtype)


def gaussian_with(stream_key, extent, deviation, reach, pieces, heavy, held_as=jnp.bfloat16):
    values = deviation * jax.random.normal(stream_key, extent, jnp.float32)
    if pieces:
        values = values * shard_levels(stream_key, extent, pieces, -0.22, 0.18)
    return jnp.clip(spiked(values, jax.random.fold_in(stream_key, 3), *heavy), -reach, reach).astype(held_as)


def setup_inputs(seed: int = 0, part: int = 0) -> dict:
    streams_of = jax.random.split(jax.random.key(seed), 6)
    own_keys = jax.random.split(jax.random.fold_in(streams_of[5], part), 6)
    return {
        "grads": gaussian_with(own_keys[0], (N_GRP, D, KV), 1.0, 6.0, ((0, 8),), (0, 1, 8, 2.0)),
        "weight": centred(own_keys[1], (D, KV), 0.04, 0.625),
        "moment1": centred(own_keys[2], (D, KV), 0.15, 2.0, ((0, 8),), jnp.float32),
        "moment2": jnp.clip(jnp.exp(math.log(0.04) - 5.9914646 * jax.random.uniform(own_keys[3], (D, KV), jnp.float32) ** shard_levels(own_keys[3], (D, KV), ((0, 8),), -0.2, 0.2)), 0.0001, 0.04),
        "step": jax.random.randint(streams_of[4], (1,), 1, 9).astype(jnp.int32),
    }


def reference(grads, weight, moment1, moment2, step):
    average = lax.optimization_barrier(jnp.sum(grads.astype(jnp.float32), axis=0)) / N_GRP
    new_moment1 = 0.9 * moment1 + 0.1 * average
    new_moment2 = 0.999 * moment2 + 0.001 * average * average
    step_count = step[0].astype(jnp.float32)
    first_hat = new_moment1 / (1.0 - jnp.power(jnp.float32(0.9), step_count))
    second_hat = new_moment2 / (1.0 - jnp.power(jnp.float32(0.999), step_count))
    updated = weight.astype(jnp.float32) * (1.0 - 0.25 * 0.1) - 0.25 * first_hat / (jnp.sqrt(second_hat) + 1e-08)
    return (updated.astype(jnp.bfloat16), new_moment1, new_moment2)
```

```python
import functools

import jax
import jax.numpy as jnp
from jax import lax
from jax.sharding import PartitionSpec as P


def grid_of(size):
    cores = 2 if size % 2 == 0 else 1
    chips = size // cores
    width = max(d for d in range(1, chips + 1) if chips % d == 0 and d * d <= chips)
    return chips // width, width, cores


def adamw_rows(average, moment1, moment2, owned_rows, step_count):
    new_moment1 = 0.9 * moment1 + 0.1 * average
    new_moment2 = 0.999 * moment2 + 0.001 * average * average
    first_hat = new_moment1 / (1.0 - jnp.power(jnp.float32(0.9), step_count))
    second_hat = new_moment2 / (1.0 - jnp.power(jnp.float32(0.999), step_count))
    updated = owned_rows.astype(jnp.float32) * (1.0 - 0.25 * 0.1) - 0.25 * first_hat / (
        jnp.sqrt(second_hat) + 1e-08
    )
    return (updated.astype(jnp.bfloat16), new_moment1, new_moment2)


def shards(size, grads, weight, moment1, moment2, step):
    ny, nx, nc = grid_of(size)
    f32, bf16 = jnp.float32, jnp.bfloat16
    local = grads[0]
    rows, width = moment1.shape
    half = width // 2
    cols = {"a": (0, half), "b": (half, width)}
    me = lax.axis_index("grp")
    my_y, my_x, my_c = me // (nx * nc), me // nc % nx, me % nc

    def flat(y, x, c):
        return (y % ny * nx + x % nx) * nc + c % nc

    def shift(dy, dx, dc):
        return [
            (flat(y, x, c), flat(y + dy, x + dx, c + dc))
            for y in range(ny)
            for x in range(nx)
            for c in range(nc)
        ]

    def send(value, dy=0, dx=0, dc=0):
        return lax.ppermute(value, "grp", shift(dy, dx, dc))

    def block(dy, dx, dc):
        first = flat(my_y + dy, my_x + dx, my_c + dc) * rows
        return lax.dynamic_slice_in_dim(local, first, rows, 0)

    ys, xs, cs = range(1, ny), range(1, nx), range(1, nc)

    def chip_sum(dy, dx):
        arrived = [send(block(dy, dx, dc), dc=dc) for dc in cs]
        return sum((a.astype(f32) for a in arrived), block(dy, dx, 0).astype(f32))

    def part(value, name):
        return value[:, cols[name][0] : cols[name][1]]

    diag = {(j, i): chip_sum(j, i) for j in ys for i in xs}
    diag_a = {k: send(part(v, "a").astype(bf16), dx=k[1]) for k, v in diag.items()}
    diag_b = {k: send(part(v, "b").astype(bf16), dy=k[0]) for k, v in diag.items()}
    by_x = {i: chip_sum(0, i) for i in xs}
    by_y = {j: chip_sum(j, 0) for j in ys}
    plain_a = [send(part(by_x[i], "a").astype(bf16), dx=i) for i in xs]
    plain_b = [send(part(by_y[j], "b").astype(bf16), dy=j) for j in ys]
    own = chip_sum(0, 0)
    aug_a = [
        send(
            sum((diag_a[j, i].astype(f32) for i in xs), part(by_y[j], "a")).astype(bf16),
            dy=j,
        )
        for j in ys
    ]
    aug_b = [
        send(
            sum((diag_b[j, i].astype(f32) for j in ys), part(by_x[i], "b")).astype(bf16),
            dx=i,
        )
        for i in xs
    ]
    total = {
        "a": sum((v.astype(f32) for v in plain_a + aug_a), part(own, "a")),
        "b": sum((v.astype(f32) for v in plain_b + aug_b), part(own, "b")),
    }

    step_count = step[0].astype(f32)
    owned = lax.dynamic_slice_in_dim(weight, me * rows, rows, 0)
    done = {
        name: adamw_rows(
            total[name] / size,
            part(moment1, name),
            part(moment2, name),
            part(owned, name),
            step_count,
        )
        for name in ("a", "b")
    }
    new1 = jnp.concatenate([done["a"][1], done["b"][1]], axis=1)
    new2 = jnp.concatenate([done["a"][2], done["b"][2]], axis=1)

    out = jnp.zeros(local.shape, bf16)

    def place(out, value, name, dy, dx, dc):
        first = flat(my_y + dy, my_x + dx, my_c + dc) * rows
        return lax.dynamic_update_slice(out, value, (first, cols[name][0]))

    held = {}
    for name in ("a", "b"):
        held[name, 0, 0] = done[name][0]
    for j in ys:
        held["a", -j, 0] = send(held["a", 0, 0], dy=j)
    for i in xs:
        held["b", 0, -i] = send(held["b", 0, 0], dx=i)
    for i in xs:
        held["a", 0, -i] = send(held["a", 0, 0], dx=i)
    for j in ys:
        held["b", -j, 0] = send(held["b", 0, 0], dy=j)
    for j in ys:
        for i in xs:
            held["a", -j, -i] = send(held["a", -j, 0], dx=i)
            held["b", -j, -i] = send(held["b", 0, -i], dy=j)
    for (name, dy, dx), value in held.items():
        out = place(out, value, name, dy, dx, 0)
        for dc in cs:
            out = place(out, send(value, dc=dc), name, dy, dx, -dc)
    return (out, new1, new2)


def solution(mesh):
    return jax.shard_map(
        functools.partial(shards, mesh.shape["grp"]),
        mesh=mesh,
        in_specs=(P("grp", "rest", None), P("rest", None), P("grp", "rest"), P("grp", "rest"), P()),
        out_specs=(P("rest", None), P("grp", "rest"), P("grp", "rest")),
        check_vma=False,
    )
```
